32 devices in a mesh: grp: 2 (over y), slab: 4 (over z), head: 2 (over x), seq: 2 (over core).
Axes of the slice: x: 2, y: 2, z: 4, core: 2. Of those that a mesh axis runs over, the one named last changes fastest.
Arguments:
- queries: bfloat16 [1024, 5120], P(('grp', 'seq'), 'head'), parts along dimension 0, may hold values from -140 to 140
- query_gain: float32 [5120], P('head'), may hold values from 1.5 to 3
- cache_keys: bfloat16 [4096, 5120], P(('grp', 'slab'), 'head'), parts along dimension 0, may hold values from -120 to 120
- cache_values: bfloat16 [4096, 5120], P(('grp', 'slab'), 'head'), parts along dimension 0, may hold values from -6 to 6
- finished_keys: bfloat16 [1024, 5120], P(('grp', 'slab', 'seq'), 'head'), parts along dimension 0, may hold values from -6 to 6
- finished_values: bfloat16 [1024, 5120], P(('grp', 'slab', 'seq'), 'head'), parts along dimension 0, may hold values from -6 to 6
- new_keys: bfloat16 [1024, 5120], P(('grp', 'slab', 'seq'), 'head'), parts along dimension 0, may hold values from -6 to 6
- new_values: bfloat16 [1024, 5120], P(('grp', 'slab', 'seq'), 'head'), parts along dimension 0, may hold values from -6 to 6
- out_weight: bfloat16 [5120, 5120], P('head', 'slab'), may hold values from -0.25 to 0.25
- time_weight: float32 [256, 5120], P(None, ('slab', 'head')), may hold values from -0.375 to 0.375
- owner: int32 [2], P('grp'), parts along dimension 0, may hold values from 0 to 3
- step: int32 [2], P('grp'), parts along dimension 0, may hold values from 0 to 999
Outputs:
- branch: bfloat16 [1024, 5120], P(('grp', 'seq'), ('slab', 'head')), parts along dimension 0
The draws below stay inside these ranges and needn't reach their ends.
There are 2 independent parts, one for each index of `grp`. The reference program is written for one: setup_inputs(seed, part) draws one part's arguments, and reference() takes and returns one part's arrays. A program takes and returns all parts, laid end to end along the dimension named above; an argument that names none is the same for every part. Nothing has to cross between parts.
All inputs are finite; a program needn't handle non-finite values.
Results may differ from the reference program's by a relative error of at most 0.012.
Values may be sent and summed in bfloat16 or wider, within the bound.
A program may use at most 64 MiB of HBM per device.

```python
import math
import jax
import jax.numpy as jnp
from jax import lax

D = 5120
HEADS = 40
HD = 128
FREQ = 256
SPAN = 512
CACHE = 2048
N_SLAB = 4


def draw_cache_keys(key, part):
    shape_pair = (SPAN * N_SLAB, HEADS * HD)
    entries = jnp.clip(jax.random.normal(jax.random.fold_in(key, 11), shape_pair, jnp.float32), -4.5, 4.5)
    return entries.astype(jnp.bfloat16)


def draw_queries(key, part):
    width_total = HEADS * HD
    shape_pair = (SPAN, width_total)
    row_scale = jnp.exp(jax.random.uniform(jax.random.fold_in(key, 21), (SPAN, 1), jnp.float32, jnp.log(0.5), jnp.log(5.0)))
    column_rise = 3.0 ** (jnp.arange(width_total, dtype=jnp.float32) / (width_total - 1))
    jitter = jnp.exp(jax.random.uniform(jax.random.fold_in(key, 22), (width_total,), jnp.float32, jnp.log(0.5), jnp.log(2.0)))
    entries = jnp.clip(jax.random.normal(jax.random.fold_in(key, 23), shape_pair, jnp.float32), -4.5, 4.5)
    entries = entries * row_scale * column_rise * jitter
    return entries.astype(jnp.bfloat16)


def shard_levels(key, shape, cuts, least, largest):
    gain, own = 1.0, jax.random.fold_in(key, 6)
    for axis_at, blocks in cuts:
        draws = jnp.exp(jax.random.uniform(jax.random.fold_in(own, axis_at), (blocks,), jnp.float32, least / len(cuts), largest / len(cuts)))
        gain = gain * jnp.repeat(draws, shape[axis_at] // blocks).reshape([-1 if axis == axis_at else 1 for axis in range(len(shape))])
    return gain


def bell_draw(rng, dims, width, bound, pieces=(), kind=jnp.bfloat16):
    values = width * jax.random.normal(rng, dims, jnp.float32)
    if pieces:
        values = values * shard_levels(rng, dims, pieces, -0.22, 0.18)
    return jnp.clip(values, -bound, bound).astype(kind)


def setup_inputs(seed: int = 0, part: int = 0) -> dict:
    arg_keys = jax.random.split(jax.random.key(seed), 13)
    own_keys = jax.random.split(jax.random.fold_in(arg_keys[12], part), 13)
    return {
        "queries": draw_queries(jax.random.fold_in(jax.random.fold_in(arg_keys[12], part), 71), part),
        "query_gain": jnp.clip(jnp.exp(math.log(3.0) - 0.6931472 * jax.random.uniform(arg_keys[1], (HEADS * HD,), jnp.float32) ** shard_levels(arg_keys[1], (HEADS * HD,), ((0, 2),), -0.2, 0.2)), 1.5, 3.0),
        "cache_keys": draw_cache_keys(jax.random.fold_in(jax.random.fold_in(arg_keys[12], part), 71), part),
        "cache_values": bell_draw(own_keys[3], (CACHE, HEADS * HD), 1.0, 6.0, ((0, 4), (1, 2))),
        "finished_keys": bell_draw(own_keys[4], (SPAN, HEADS * HD), 1.0, 6.0, ((0, 8), (1, 2))),
        "finished_values": bell_draw(own_keys[5], (SPAN, HEADS * HD), 1.0, 6.0, ((0, 8), (1, 2))),
        "new_keys": bell_draw(own_keys[6], (SPAN, HEADS * HD), 1.0, 6.0, ((0, 8), (1, 2))),
        "new_values": bell_draw(own_keys[7], (SPAN, HEADS * HD), 1.0, 6.0, ((0, 8), (1, 2))),
        "out_weight": bell_draw(arg_keys[8], (HEADS * HD, D), (HEADS * HD // 8) ** -0.5, 0.25, ((0, 2), (1, 4))),
        "time_weight": bell_draw(arg_keys[9], (FREQ, D), FREQ ** -0.5, 0.375, ((1, 8),), jnp.float32),
        "owner": jax.random.randint(own_keys[10], (1,), 0, N_SLAB).astype(jnp.int32),
        "step": jax.random.randint(own_keys[11], (1,), 0, 1000).astype(jnp.int32),
    }


EPSILON = 1e-06

def reference(queries, query_gain, cache_keys, cache_values, finished_keys, finished_values, new_keys, new_values, out_weight, time_weight, owner, step):
    query_float = queries.astype(jnp.float32)
    inverse = lax.rsqrt(lax.optimization_barrier(jnp.mean(query_float * query_float, axis=1)) + EPSILON)
    normed = (query_float * inverse[:, None] * query_gain).astype(jnp.bfloat16)
    start_row = (owner[0] * SPAN).astype(jnp.int32)
    swapped_keys = lax.dynamic_update_slice(cache_keys, finished_keys, (start_row, jnp.int32(0)))
    swapped_values = lax.dynamic_update_slice(cache_values, finished_values, (start_row, jnp.int32(0)))
    all_keys = jnp.concatenate([swapped_keys, new_keys], axis=0)
    all_values = jnp.concatenate([swapped_values, new_values], axis=0)
    total_rows = CACHE + SPAN
    query_heads = normed.reshape(SPAN, HEADS, HD).transpose(1, 0, 2)
    key_heads = all_keys.reshape(total_rows, HEADS, HD).transpose(1, 0, 2)
    value_heads = all_values.reshape(total_rows, HEADS, HD).transpose(1, 0, 2)
    score_scale = 1.0 / HD ** 0.5

    def one_head(head_items):
        query_head, key_head, value_head = head_items
        scores = jnp.dot(query_head, key_head.T, preferred_element_type=jnp.float32) * score_scale
        row_top = lax.optimization_barrier(jnp.max(scores, axis=1, keepdims=True))
        raw_weights = jnp.exp(scores - row_top)
        row_mass = lax.optimization_barrier(jnp.sum(raw_weights, axis=1, keepdims=True))
        weighted = jnp.dot(raw_weights.astype(jnp.bfloat16), value_head, preferred_element_type=jnp.float32)
        return (weighted / row_mass).astype(jnp.bfloat16)
    attended = lax.map(one_head, (query_heads, key_heads, value_heads))
    weight_heads = out_weight.reshape(HEADS, HD, D)
    projected = jnp.einsum('hrd,hdc->rc', attended.astype(jnp.float32), weight_heads.astype(jnp.float32))
    half = FREQ // 2
    frequency = jnp.exp(-jnp.log(10000.0) * jnp.arange(half, dtype=jnp.float32) / half)
    phases = step[0].astype(jnp.float32) * frequency
    embedding = jnp.concatenate([jnp.cos(phases), jnp.sin(phases)])
    time_gate = 1.0 + jnp.dot(embedding, time_weight, precision=lax.Precision.HIGHEST)
    return (time_gate * projected).astype(jnp.bfloat16)
```

```python
import functools
import math

import jax
import jax.numpy as jnp
from jax import lax
from jax.experimental import pallas as pl
from jax.experimental.pallas import tpu as pltpu
from jax.sharding import PartitionSpec as P

HEADS = 40
HD = 128
EPSILON = 1e-06
LOW = -1e30
LAG = 3
MESH = pl.DeviceIdType.MESH
F32 = jnp.float32
BF16 = jnp.bfloat16


def kernel(
    dims,
    aligned,
    q_ref,
    gain_ref,
    ck_ref,
    cv_ref,
    fk_ref,
    fv_ref,
    nk_ref,
    nv_ref,
    w_ref,
    tw_ref,
    owner_ref,
    step_ref,
    out_ref,
    q,
    qg,
    gain,
    kc,
    vc,
    kf,
    vf,
    w,
    tw,
    squares,
    scale,
    own_o,
    own_s,
    pre_o,
    pre_s,
    suf_o,
    suf_s,
    right_o,
    right_s,
    left_o,
    left_s,
    acc,
    gate,
    xs,
    xr,
    load_sem,
    fresh_sem,
    fresh_send,
    fresh_recv,
    sq_send,
    sq_recv,
    right_send,
    right_recv,
    left_send,
    left_recv,
    x_send,
    x_recv,
):
    n, heads_n, seq_n = dims
    rows, width = q_ref.shape
    hcount = width // HD
    z = lax.axis_index("slab")
    hx = lax.axis_index("head")
    sq = lax.axis_index("seq")

    loads = [
        pltpu.make_async_copy(src, dst, load_sem.at[i])
        for i, (src, dst) in enumerate(
            [(q_ref, q), (gain_ref, gain), (ck_ref, kc), (cv_ref, vc), (w_ref, w), (tw_ref, tw)]
        )
    ]
    for c in loads:
        c.start()
    fresh_src = [(fk_ref, kf, 0), (nk_ref, kf, 1), (fv_ref, vf, 0), (nv_ref, vf, 1)]
    fresh_local = []
    for i, (src, dst, part) in enumerate(fresh_src):
        c = pltpu.make_async_copy(src, dst.at[sq, part], fresh_sem.at[i])
        c.start()
        fresh_local.append(c)

    barrier = pltpu.get_barrier_semaphore()
    for d in range(1, seq_n):
        pl.semaphore_signal(
            barrier, inc=1, device_id={"seq": lax.rem(sq + d, seq_n)}, device_id_type=MESH
        )
    for d in range(1, heads_n):
        pl.semaphore_signal(
            barrier, inc=1, device_id={"head": lax.rem(hx + d, heads_n)}, device_id_type=MESH
        )

    @pl.when(z > 0)
    def _():
        pl.semaphore_signal(barrier, inc=1, device_id={"slab": z - 1}, device_id_type=MESH)

    @pl.when(z < n - 1)
    def _():
        pl.semaphore_signal(barrier, inc=1, device_id={"slab": z + 1}, device_id_type=MESH)

    ends = (z == 0).astype(jnp.int32) + (z == n - 1).astype(jnp.int32)
    pl.semaphore_wait(barrier, seq_n - 1 + heads_n - 1 + 2 - ends)

    fresh_remote = []
    for d in range(1, seq_n):
        for i, (src, dst, part) in enumerate(fresh_src):
            c = pltpu.make_async_remote_copy(
                src_ref=src,
                dst_ref=dst.at[sq, part],
                send_sem=fresh_send.at[d - 1, i],
                recv_sem=fresh_recv.at[d - 1, i],
                device_id={"seq": lax.rem(sq + d, seq_n)},
                device_id_type=MESH,
            )
            c.start()
            fresh_remote.append(c)

    loads[0].wait()
    loads[1].wait()

    def squares_step(h, total):
        cols = pl.ds(pl.multiple_of(h * HD, HD), HD)
        x = q[:, cols].astype(F32)
        qg[:, cols] = (x * gain[:, cols]).astype(BF16)
        return total + x * x

    total = lax.fori_loop(0, hcount, squares_step, jnp.zeros((rows, HD), F32))
    row_total = jnp.sum(total.T, axis=0, keepdims=True)
    squares[hx] = jnp.broadcast_to(row_total, (8, rows))
    loads[2].wait()
    loads[3].wait()
    sq_copies = []
    for d in range(1, heads_n):
        c = pltpu.make_async_remote_copy(
            src_ref=squares.at[hx],
            dst_ref=squares.at[hx],
            send_sem=sq_send.at[d - 1],
            recv_sem=sq_recv.at[d - 1],
            device_id={"head": lax.rem(hx + d, heads_n)},
            device_id_type=MESH,
        )
        c.start()
        sq_copies.append(c)
    for c in fresh_local:
        c.wait()
    for c in fresh_remote:
        c.wait_recv()
    for c in sq_copies:
        c.wait_recv()
    norm_total = jnp.sum(squares[...], axis=0)
    scale[...] = lax.rsqrt(norm_total / (HEADS * HD) + EPSILON) * (
        math.log2(math.e) / HD**0.5
    )
    loads[4].wait()
    loads[5].wait()

    def send(h, direction):
        if direction > 0:
            pairs, ss, rs = ((right_o, pre_o), (right_s, pre_s)), right_send, right_recv
        else:
            pairs, ss, rs = ((left_o, suf_o), (left_s, suf_s)), left_send, left_recv
        return [
            pltpu.make_async_remote_copy(
                src_ref=src.at[h],
                dst_ref=dst.at[h],
                send_sem=ss.at[h, i],
                recv_sem=rs.at[h, i],
                device_id={"slab": z + direction},
                device_id_type=MESH,
            )
            for i, (src, dst) in enumerate(pairs)
        ]

    @pl.when(z == 0)
    def _():
        pre_o[...] = jnp.zeros_like(pre_o)
        pre_s[:, 0:1, :] = jnp.full((hcount, 1, rows), LOW, F32)
        pre_s[:, 1:2, :] = jnp.zeros((hcount, 1, rows), F32)

    @pl.when(z == n - 1)
    def _():
        suf_o[...] = jnp.zeros_like(suf_o)
        suf_s[:, 0:1, :] = jnp.full((hcount, 1, rows), LOW, F32)
        suf_s[:, 1:2, :] = jnp.zeros((hcount, 1, rows), F32)

    fresh_rows = seq_n * 2 * fk_ref.shape[0]
    lag_end = LAG * jnp.maximum(z, n - 1 - z)

    def combine(h, other_o, other_s, dest_o, dest_s):
        m_a, l_a = own_s[h, 0:1], own_s[h, 1:2]
        m_b, l_b = other_s[h, 0:1], other_s[h, 1:2]
        top = jnp.maximum(m_a, m_b)
        e_a, e_b = jnp.exp2(m_a - top), jnp.exp2(m_b - top)
        dest_o[h] = (own_o[h] * e_a + other_o[h].astype(F32) * e_b).astype(BF16)
        dest_s[h, 0:1] = top
        dest_s[h, 1:2] = l_a * e_a + l_b * e_b

    def body(t, carry):
        @pl.when(t < hcount)
        def _():
            h = t
            cols = pl.ds(pl.multiple_of(h * HD, HD), HD)
            penalty = jnp.where(
                jnp.full((1, rows), owner_ref[0], jnp.int32) == z, F32(LOW), F32(0.0)
            )
            q_head = qg[:, cols]
            s_row = scale[0:1]
            nt = (((1,), (1,)), ((), ()))
            tn = (((0,), (0,)), ((), ()))
            s_c = (
                lax.dot_general(kc[:, cols], q_head, nt, preferred_element_type=F32) * s_row
                + penalty
            )
            k_fresh = kf[:, :, :, cols].reshape(fresh_rows, HD)
            v_fresh = vf[:, :, :, cols].reshape(fresh_rows, HD)
            s_f = lax.dot_general(k_fresh, q_head, nt, preferred_element_type=F32) * s_row
            top = jnp.maximum(
                jnp.max(s_c, axis=0, keepdims=True), jnp.max(s_f, axis=0, keepdims=True)
            )
            p_c = jnp.exp2(s_c - top)
            p_f = jnp.exp2(s_f - top)
            own_s[h, 0:1] = top
            own_s[h, 1:2] = jnp.sum(p_c, axis=0, keepdims=True) + jnp.sum(
                p_f, axis=0, keepdims=True
            )
            own_o[h] = lax.dot_general(
                vc[:, cols], p_c.astype(BF16), tn, preferred_element_type=F32
            ) + lax.dot_general(v_fresh, p_f.astype(BF16), tn, preferred_element_type=F32)

        hp = t - LAG * z
        in_p = (hp >= 0) & (hp < hcount)
        hs = t - LAG * (n - 1 - z)
        in_s = (hs >= 0) & (hs < hcount)

        @pl.when(in_p & (z > 0))
        def _():
            for c in send(hp, 1):
                c.wait_recv()

        @pl.when(in_p & (z < n - 1))
        def _():
            combine(hp, pre_o, pre_s, right_o, right_s)

        @pl.when(in_s & (z < n - 1))
        def _():
            for c in send(hs, -1):
                c.wait_recv()

        @pl.when(in_s & (z > 0))
        def _():
            combine(hs, suf_o, suf_s, left_o, left_s)

        @pl.when(in_p & (z < n - 1))
        def _():
            for c in send(hp, 1):
                c.start()

        @pl.when(in_s & (z > 0))
        def _():
            for c in send(hs, -1):
                c.start()

        if aligned:

            @pl.when(t == hcount - 1)
            def _():
                half = tw.shape[0] // 2
                j = lax.broadcasted_iota(jnp.int32, (half, HD), 0).astype(F32)
                frequency = jnp.exp(F32(-math.log(10000.0)) * j / half)
                phases = jnp.full((half, HD), step_ref[0], jnp.int32).astype(F32) * frequency
                cos, sin = jnp.cos(phases), jnp.sin(phases)
                for c in range(tw.shape[1] // HD):
                    cols = slice(c * HD, (c + 1) * HD)
                    terms = tw[:half, cols] * cos + tw[half:, cols] * sin
                    gate[:, cols] = 1.0 + jnp.sum(terms, axis=0, keepdims=True)

        hf = t - lag_end

        @pl.when((hf >= 0) & (hf < hcount))
        def _():
            h = hf
            m_a, m_b, m_c = own_s[h, 0:1], pre_s[h, 0:1], suf_s[h, 0:1]
            top = jnp.maximum(m_a, jnp.maximum(m_b, m_c))
            e_a, e_b, e_c = jnp.exp2(m_a - top), jnp.exp2(m_b - top), jnp.exp2(m_c - top)
            mass = own_s[h, 1:2] * e_a + pre_s[h, 1:2] * e_b + suf_s[h, 1:2] * e_c
            total_o = (
                own_o[h] * e_a + pre_o[h].astype(F32) * e_b + suf_o[h].astype(F32) * e_c
            )
            attended = (total_o / mass).astype(BF16)
            term = lax.dot_general(
                attended,
                w[pl.ds(pl.multiple_of(h * HD, HD), HD), :],
                (((0,), (0,)), ((), ())),
                preferred_element_type=F32,
            )

            @pl.when(h == 0)
            def _():
                acc[...] = term

            @pl.when(h > 0)
            def _():
                acc[...] += term

        return carry

    lax.fori_loop(0, hcount + LAG * (n - 1), body, 0)

    if aligned:
        cp = out_ref.shape[1]
        blocks = x_send.shape[1]
        block = rows // blocks
        x_copies = []
        for b in range(blocks):
            part = slice(b * block, (b + 1) * block)
            for d in range(1, heads_n):
                peer = lax.rem(hx + d, heads_n)
                cols = pl.ds(pl.multiple_of(peer * cp, HD), cp)
                xs[d - 1, b] = acc[part, cols].astype(BF16)
                c = pltpu.make_async_remote_copy(
                    src_ref=xs.at[d - 1, b],
                    dst_ref=xr.at[d - 1, b],
                    send_sem=x_send.at[d - 1, b],
                    recv_sem=x_recv.at[d - 1, b],
                    device_id={"head": peer},
                    device_id_type=MESH,
                )
                c.start()
                x_copies.append((b, d, c))
        mine = pl.ds(pl.multiple_of(hx * cp, HD), cp)
        for b in range(blocks):
            part = slice(b * block, (b + 1) * block)
            summed = acc[part, mine]
            for bb, d, c in x_copies:
                if bb == b:
                    c.wait_recv()
                    summed = summed + xr[d - 1, b].astype(F32)
            out_ref[part, :] = (summed * gate[0:1]).astype(out_ref.dtype)
        for b, d, c in x_copies:
            c.wait_send()
    else:
        out_ref[...] = acc[...]

    for c in fresh_remote + sq_copies:
        c.wait_send()

    def drain(h, carry):
        @pl.when(z < n - 1)
        def _():
            for c in send(h, 1):
                c.wait_send()

        @pl.when(z > 0)
        def _():
            for c in send(h, -1):
                c.wait_send()

        return carry

    lax.fori_loop(0, hcount, drain, 0)


def local(sizes, *args):
    (
        queries,
        query_gain,
        cache_keys,
        cache_values,
        finished_keys,
        finished_values,
        new_keys,
        new_values,
        out_weight,
        time_weight,
        owner,
        step,
    ) = args
    n, heads_n, seq_n = sizes
    rows, width = queries.shape
    hcount = width // HD
    cached, fresh = cache_keys.shape[0], finished_keys.shape[0]
    columns, cp = out_weight.shape[1], time_weight.shape[1]
    freq = time_weight.shape[0]
    aligned = cp % HD == 0
    blocks = 4
    any_spec = pl.BlockSpec(memory_space=pl.ANY)
    smem = pl.BlockSpec(memory_space=pltpu.SMEM)
    vmem = pl.BlockSpec(memory_space=pltpu.VMEM)
    dma = pltpu.SemaphoreType.DMA
    xcount = max(heads_n - 1, 1)
    stat = (hcount, 2, rows)
    part = (hcount, HD, rows)
    result = pl.pallas_call(
        functools.partial(kernel, sizes, aligned),
        out_shape=jax.ShapeDtypeStruct(
            (rows, cp if aligned else columns), BF16 if aligned else F32
        ),
        in_specs=[any_spec] * 10 + [smem] * 2,
        out_specs=vmem,
        scratch_shapes=[
            pltpu.VMEM((rows, width), BF16),
            pltpu.VMEM((rows, width), BF16),
            pltpu.VMEM((1, width), F32),
            pltpu.VMEM((cached, width), BF16),
            pltpu.VMEM((cached, width), BF16),
            pltpu.VMEM((seq_n, 2, fresh, width), BF16),
            pltpu.VMEM((seq_n, 2, fresh, width), BF16),
            pltpu.VMEM((width, columns), BF16),
            pltpu.VMEM((freq, cp), F32),
            pltpu.VMEM((heads_n, 8, rows), F32),
            pltpu.VMEM((8, rows), F32),
            pltpu.VMEM(part, F32),
            pltpu.VMEM(stat, F32),
            pltpu.VMEM(part, BF16),
            pltpu.VMEM(stat, F32),
            pltpu.VMEM(part, BF16),
            pltpu.VMEM(stat, F32),
            pltpu.VMEM(part, BF16),
            pltpu.VMEM(stat, F32),
            pltpu.VMEM(part, BF16),
            pltpu.VMEM(stat, F32),
            pltpu.VMEM((rows, columns), F32),
            pltpu.VMEM((1, cp), F32),
            pltpu.VMEM((xcount, blocks, rows // blocks, cp), BF16),
            pltpu.VMEM((xcount, blocks, rows // blocks, cp), BF16),
            dma((6,)),
            dma((4,)),
            dma((max(seq_n - 1, 1), 4)),
            dma((max(seq_n - 1, 1), 4)),
            dma((xcount,)),
            dma((xcount,)),
            dma((hcount, 2)),
            dma((hcount, 2)),
            dma((hcount, 2)),
            dma((hcount, 2)),
            dma((xcount, blocks)),
            dma((xcount, blocks)),
        ],
        compiler_params=pltpu.CompilerParams(
            collective_id=0, has_side_effects=True, vmem_limit_bytes=60 * 1024 * 1024
        ),
        name="sweep_attention",
    )(
        queries,
        query_gain.reshape(1, width),
        cache_keys,
        cache_values,
        finished_keys,
        finished_values,
        new_keys,
        new_values,
        out_weight,
        time_weight,
        owner,
        step,
    )
    if aligned:
        return result
    summed = lax.psum_scatter(result, "head", scatter_dimension=1, tiled=True)
    half = freq // 2
    frequency = jnp.exp(-jnp.log(10000.0) * jnp.arange(half, dtype=F32) / half)
    phases = step[0].astype(F32) * frequency
    embedding = jnp.concatenate([jnp.cos(phases), jnp.sin(phases)])
    time_gate = 1.0 + jnp.dot(embedding, time_weight, precision=lax.Precision.HIGHEST)
    return (time_gate * summed).astype(BF16)


def solution(mesh):
    in_specs = (
        P(("grp", "seq"), "head"),
        P("head"),
        P(("grp", "slab"), "head"),
        P(("grp", "slab"), "head"),
        P(("grp", "slab", "seq"), "head"),
        P(("grp", "slab", "seq"), "head"),
        P(("grp", "slab", "seq"), "head"),
        P(("grp", "slab", "seq"), "head"),
        P("head", "slab"),
        P(None, ("slab", "head")),
        P("grp"),
        P("grp"),
    )
    out_specs = P(("grp", "seq"), ("slab", "head"))
    sizes = (mesh.shape["slab"], mesh.shape["head"], mesh.shape["seq"])
    return jax.shard_map(
        functools.partial(local, sizes),
        mesh=mesh,
        in_specs=in_specs,
        out_specs=out_specs,
        check_vma=False,
    )
```

```python
import functools
import math

import jax
import jax.numpy as jnp
from jax import lax
from jax.experimental import pallas as pl
from jax.experimental.pallas import tpu as pltpu
from jax.sharding import PartitionSpec as P

HEADS = 40
HD = 128
EPSILON = 1e-06
LOW = -1e30
LAG = 4
MESH = pl.DeviceIdType.MESH
F32 = jnp.float32
BF16 = jnp.bfloat16


def kernel(
    dims,
    aligned,
    q_ref,
    gain_ref,
    ck_ref,
    cv_ref,
    fk_ref,
    fv_ref,
    nk_ref,
    nv_ref,
    w_ref,
    tw_ref,
    owner_ref,
    step_ref,
    out_ref,
    q,
    qg,
    gain,
    kc,
    vc,
    kf,
    vf,
    w,
    tw,
    squares,
    scale,
    own_o,
    own_s,
    pre_o,
    pre_s,
    suf_o,
    suf_s,
    right_o,
    right_s,
    left_o,
    left_s,
    att,
    acc,
    gate,
    xs,
    xr,
    load_sem,
    fresh_sem,
    fresh_send,
    fresh_recv,
    sq_send,
    sq_recv,
    right_send,
    right_recv,
    left_send,
    left_recv,
    x_send,
    x_recv,
):
    n, heads_n, seq_n = dims
    rows, width = q_ref.shape
    hcount = width // HD
    z = lax.axis_index("slab")
    hx = lax.axis_index("head")
    sq = lax.axis_index("seq")

    groups = rows // HD
    chunks = groups * hcount
    loads = [
        pltpu.make_async_copy(src, dst, load_sem.at[i])
        for i, (src, dst) in enumerate(
            [(q_ref, q), (gain_ref, gain), (ck_ref, kc), (cv_ref, vc), (w_ref, w), (tw_ref, tw)]
        )
    ]
    loads[0].start()
    loads[1].start()
    barrier = pltpu.get_barrier_semaphore()
    for d in range(1, seq_n):
        pl.semaphore_signal(
            barrier, inc=1, device_id={"seq": lax.rem(sq + d, seq_n)}, device_id_type=MESH
        )
    for d in range(1, heads_n):
        pl.semaphore_signal(
            barrier, inc=1, device_id={"head": lax.rem(hx + d, heads_n)}, device_id_type=MESH
        )

    @pl.when(z > 0)
    def _():
        pl.semaphore_signal(barrier, inc=1, device_id={"slab": z - 1}, device_id_type=MESH)

    @pl.when(z < n - 1)
    def _():
        pl.semaphore_signal(barrier, inc=1, device_id={"slab": z + 1}, device_id_type=MESH)

    def clear(o_ref, s_ref):
        o_ref[...] = jnp.zeros_like(o_ref)
        s_ref[:, 0:1, :] = jnp.full((chunks, 1, HD), LOW, F32)
        s_ref[:, 1:2, :] = jnp.zeros((chunks, 1, HD), F32)

    @pl.when(z == 0)
    def _():
        clear(pre_o, pre_s)

    @pl.when(z == n - 1)
    def _():
        clear(suf_o, suf_s)

    ends = (z == 0).astype(jnp.int32) + (z == n - 1).astype(jnp.int32)
    pl.semaphore_wait(barrier, seq_n - 1 + heads_n - 1 + 2 - ends)

    fresh_src = [(fk_ref, kf, 0), (nk_ref, kf, 1), (fv_ref, vf, 0), (nv_ref, vf, 1)]
    fresh_remote = []
    for d in range(1, seq_n):
        for i, (src, dst, part) in enumerate(fresh_src):
            c = pltpu.make_async_remote_copy(
                src_ref=src,
                dst_ref=dst.at[sq, part],
                send_sem=fresh_send.at[d - 1, i],
                recv_sem=fresh_recv.at[d - 1, i],
                device_id={"seq": lax.rem(sq + d, seq_n)},
                device_id_type=MESH,
            )
            c.start()
            fresh_remote.append(c)

    loads[0].wait()
    loads[1].wait()
    loads[5].start()
    loads[2].start()
    loads[3].start()
    fresh_local = []
    for i, (src, dst, part) in enumerate(fresh_src):
        c = pltpu.make_async_copy(src, dst.at[sq, part], fresh_sem.at[i])
        c.start()
        fresh_local.append(c)
    loads[4].start()

    def squares_step(h, total):
        cols = pl.ds(pl.multiple_of(h * HD, HD), HD)
        x = q[:, cols].astype(F32)
        qg[:, cols] = (x * gain[cols][None, :]).astype(BF16)
        return total + x * x

    total = lax.fori_loop(0, hcount, squares_step, jnp.zeros((rows, HD), F32))
    row_total = jnp.sum(total.T, axis=0, keepdims=True)
    squares[hx] = jnp.broadcast_to(row_total, (8, rows))
    loads[5].wait()
    sq_copies = []
    for d in range(1, heads_n):
        c = pltpu.make_async_remote_copy(
            src_ref=squares.at[hx],
            dst_ref=squares.at[hx],
            send_sem=sq_send.at[d - 1],
            recv_sem=sq_recv.at[d - 1],
            device_id={"head": lax.rem(hx + d, heads_n)},
            device_id_type=MESH,
        )
        c.start()
        sq_copies.append(c)
    if aligned:
        half = tw.shape[0] // 2
        j = lax.broadcasted_iota(jnp.int32, (half, HD), 0).astype(F32)
        frequency = jnp.exp(F32(-math.log(10000.0)) * j / half)
        phases = jnp.full((half, HD), step_ref[0], jnp.int32).astype(F32) * frequency
        cos, sin = jnp.cos(phases), jnp.sin(phases)
        for c in range(tw.shape[1] // HD):
            cols = slice(c * HD, (c + 1) * HD)
            terms = tw[:half, cols] * cos + tw[half:, cols] * sin
            gate[:, cols] = 1.0 + jnp.sum(terms, axis=0, keepdims=True)

    for c in fresh_local + loads[2:4]:
        c.wait()
    for c in fresh_remote:
        c.wait_recv()
    for c in sq_copies:
        c.wait_recv()
    norm_total = jnp.sum(squares[...], axis=0)
    scale[...] = lax.rsqrt(norm_total / (HEADS * HD) + EPSILON) * (
        math.log2(math.e) / HD**0.5
    )
    def send(h, direction):
        if direction > 0:
            pairs, ss, rs = ((right_o, pre_o), (right_s, pre_s)), right_send, right_recv
        else:
            pairs, ss, rs = ((left_o, suf_o), (left_s, suf_s)), left_send, left_recv
        return [
            pltpu.make_async_remote_copy(
                src_ref=src.at[h],
                dst_ref=dst.at[h],
                send_sem=ss.at[h, i],
                recv_sem=rs.at[h, i],
                device_id={"slab": z + direction},
                device_id_type=MESH,
            )
            for i, (src, dst) in enumerate(pairs)
        ]

    pair = 2 if hcount % 2 == 0 else 1
    fresh_rows = seq_n * 2 * fk_ref.shape[0]
    lag_end = LAG * jnp.maximum(z, n - 1 - z)

    def combine(h, other_o, other_s, dest_o, dest_s):
        m_a, l_a = own_s[h, 0:1], own_s[h, 1:2]
        m_b, l_b = other_s[h, 0:1], other_s[h, 1:2]
        top = jnp.maximum(m_a, m_b)
        e_a, e_b = jnp.exp2(m_a - top), jnp.exp2(m_b - top)
        dest_o[h] = (own_o[h] * e_a + other_o[h].astype(F32) * e_b).astype(BF16)
        dest_s[h, 0:1] = top
        dest_s[h, 1:2] = l_a * e_a + l_b * e_b

    nt = (((1,), (1,)), ((), ()))
    tn = (((0,), (0,)), ((), ()))

    def attend(h):
        cols = pl.ds(pl.multiple_of(h * HD, HD), HD)
        penalty = jnp.where(
            jnp.full((1, rows), owner_ref[0], jnp.int32) == z, F32(LOW), F32(0.0)
        )
        q_head = qg[:, cols]
        s_row = scale[0:1]
        s_c = (
            lax.dot_general(kc[:, cols], q_head, nt, preferred_element_type=F32) * s_row
            + penalty
        )
        k_fresh = kf[:, :, :, cols].reshape(fresh_rows, HD)
        v_fresh = vf[:, :, :, cols].reshape(fresh_rows, HD)
        s_f = lax.dot_general(k_fresh, q_head, nt, preferred_element_type=F32) * s_row
        top = jnp.maximum(
            jnp.max(s_c, axis=0, keepdims=True), jnp.max(s_f, axis=0, keepdims=True)
        )
        p_c = jnp.exp2(s_c - top)
        p_f = jnp.exp2(s_f - top)
        mass = jnp.sum(p_c, axis=0, keepdims=True) + jnp.sum(p_f, axis=0, keepdims=True)
        o = lax.dot_general(
            vc[:, cols], p_c.astype(BF16), tn, preferred_element_type=F32
        ) + lax.dot_general(v_fresh, p_f.astype(BF16), tn, preferred_element_type=F32)
        for g in range(groups):
            part = slice(g * HD, (g + 1) * HD)
            own_s[g * hcount + h, 0:1] = top[:, part]
            own_s[g * hcount + h, 1:2] = mass[:, part]
            own_o[g * hcount + h] = o[:, part]

    def project(g, p):
        deep = pl.ds(pl.multiple_of(p * pair * HD, HD), pair * HD)
        term = lax.dot_general(att[g, deep, :], w[deep, :], tn, preferred_element_type=F32)

        @pl.when(p == 0)
        def _():
            acc[g] = term

        @pl.when(p > 0)
        def _():
            acc[g] += term

    def exchange(g):
        copies = []
        for d in range(1, heads_n):
            copies.append(
                pltpu.make_async_remote_copy(
                    src_ref=xs.at[d - 1, g],
                    dst_ref=xr.at[d - 1, g],
                    send_sem=x_send.at[d - 1, g],
                    recv_sem=x_recv.at[d - 1, g],
                    device_id={"head": lax.rem(hx + d, heads_n)},
                    device_id_type=MESH,
                )
            )
        return copies

    def exchange_start(g):
        cp = out_ref.shape[1]
        for d, c in enumerate(exchange(g)):
            peer = lax.rem(hx + d + 1, heads_n)
            cols = pl.ds(pl.multiple_of(peer * cp, HD), cp)
            xs[d, g] = acc[g, :, cols].astype(BF16)
            c.start()

    pairs = hcount // pair
    last = (groups - 1) * hcount
    attend(0)

    def body(t, carry):
        cp_ = t - LAG * z
        in_p = (cp_ >= 0) & (cp_ < chunks)
        cs = t - LAG * (n - 1 - z)
        in_s = (cs >= 0) & (cs < chunks)

        @pl.when(in_p & (z > 0))
        def _():
            for c in send(cp_, 1):
                c.wait_recv()

        @pl.when(in_p & (z < n - 1))
        def _():
            combine(cp_, pre_o, pre_s, right_o, right_s)

        @pl.when(in_s & (z < n - 1))
        def _():
            for c in send(cs, -1):
                c.wait_recv()

        @pl.when(in_s & (z > 0))
        def _():
            combine(cs, suf_o, suf_s, left_o, left_s)

        f = t - lag_end

        @pl.when((f >= 0) & (f < chunks))
        def _():
            m_a, m_b, m_c = own_s[f, 0:1], pre_s[f, 0:1], suf_s[f, 0:1]
            top = jnp.maximum(m_a, jnp.maximum(m_b, m_c))
            e_a, e_b, e_c = jnp.exp2(m_a - top), jnp.exp2(m_b - top), jnp.exp2(m_c - top)
            mass = own_s[f, 1:2] * e_a + pre_s[f, 1:2] * e_b + suf_s[f, 1:2] * e_c
            total_o = (
                own_o[f] * e_a + pre_o[f].astype(F32) * e_b + suf_o[f].astype(F32) * e_c
            )
            h = lax.rem(f, hcount)
            att[f // hcount, pl.ds(pl.multiple_of(h * HD, HD), HD), :] = (
                total_o / mass
            ).astype(BF16)

        @pl.when(in_p & (z < n - 1))
        def _():
            for c in send(cp_, 1):
                c.start()

        @pl.when(in_s & (z > 0))
        def _():
            for c in send(cs, -1):
                c.start()

        @pl.when(t + 1 < hcount)
        def _():
            attend(t + 1)

        @pl.when(f == last)
        def _():
            loads[4].wait()

        for g in range(groups - 1):

            @pl.when((f >= last) & (f < last + pairs))
            def _(g=g):
                project(g, f - last)

            if aligned:

                @pl.when(f == last + pairs - 1)
                def _(g=g):
                    exchange_start(g)

        done = f - last + 1

        @pl.when((done > 0) & (done <= hcount) & (lax.rem(done, pair) == 0))
        def _():
            project(groups - 1, done // pair - 1)

        return carry

    lax.fori_loop(0, chunks + LAG * (n - 1), body, 0)

    if aligned:
        cp = out_ref.shape[1]
        mine = pl.ds(pl.multiple_of(hx * cp, HD), cp)
        exchange_start(groups - 1)
        for g in range(groups):
            summed = acc[g, :, mine]
            for d, c in enumerate(exchange(g)):
                c.wait_recv()
                summed = summed + xr[d, g].astype(F32)
            out_ref[g * HD : (g + 1) * HD, :] = (summed * gate[...]).astype(out_ref.dtype)
        for g in range(groups):
            for c in exchange(g):
                c.wait_send()
    else:
        for g in range(groups):
            out_ref[g * HD : (g + 1) * HD, :] = acc[g]

    for c in fresh_remote + sq_copies:
        c.wait_send()

    def drain(h, carry):
        @pl.when(z < n - 1)
        def _():
            for c in send(h, 1):
                c.wait_send()

        @pl.when(z > 0)
        def _():
            for c in send(h, -1):
                c.wait_send()

        return carry

    lax.fori_loop(0, chunks, drain, 0)


def local(sizes, *args):
    (
        queries,
        query_gain,
        cache_keys,
        cache_values,
        finished_keys,
        finished_values,
        new_keys,
        new_values,
        out_weight,
        time_weight,
        owner,
        step,
    ) = args
    n, heads_n, seq_n = sizes
    rows, width = queries.shape
    hcount = width // HD
    cached, fresh = cache_keys.shape[0], finished_keys.shape[0]
    columns, cp = out_weight.shape[1], time_weight.shape[1]
    freq = time_weight.shape[0]
    aligned = cp % HD == 0
    any_spec = pl.BlockSpec(memory_space=pl.ANY)
    smem = pl.BlockSpec(memory_space=pltpu.SMEM)
    vmem = pl.BlockSpec(memory_space=pltpu.VMEM)
    dma = pltpu.SemaphoreType.DMA
    xcount = max(heads_n - 1, 1)
    groups = rows // HD
    chunks = groups * hcount
    stat = (chunks, 2, HD)
    part = (chunks, HD, HD)
    result = pl.pallas_call(
        functools.partial(kernel, sizes, aligned),
        out_shape=jax.ShapeDtypeStruct(
            (rows, cp if aligned else columns), BF16 if aligned else F32
        ),
        in_specs=[any_spec] * 10 + [smem] * 2,
        out_specs=vmem,
        scratch_shapes=[
            pltpu.VMEM((rows, width), BF16),
            pltpu.VMEM((rows, width), BF16),
            pltpu.VMEM((width,), F32),
            pltpu.VMEM((cached, width), BF16),
            pltpu.VMEM((cached, width), BF16),
            pltpu.VMEM((seq_n, 2, fresh, width), BF16),
            pltpu.VMEM((seq_n, 2, fresh, width), BF16),
            pltpu.VMEM((width, columns), BF16),
            pltpu.VMEM((freq, cp), F32),
            pltpu.VMEM((heads_n, 8, rows), F32),
            pltpu.VMEM((8, rows), F32),
            pltpu.VMEM(part, F32),
            pltpu.VMEM(stat, F32),
            pltpu.VMEM(part, BF16),
            pltpu.VMEM(stat, F32),
            pltpu.VMEM(part, BF16),
            pltpu.VMEM(stat, F32),
            pltpu.VMEM(part, BF16),
            pltpu.VMEM(stat, F32),
            pltpu.VMEM(part, BF16),
            pltpu.VMEM(stat, F32),
            pltpu.VMEM((groups, width, HD), BF16),
            pltpu.VMEM((groups, HD, columns), F32),
            pltpu.VMEM((1, cp), F32),
            pltpu.VMEM((xcount, groups, HD, cp), BF16),
            pltpu.VMEM((xcount, groups, HD, cp), BF16),
            dma((6,)),
            dma((4,)),
            dma((max(seq_n - 1, 1), 4)),
            dma((max(seq_n - 1, 1), 4)),
            dma((xcount,)),
            dma((xcount,)),
            dma((chunks, 2)),
            dma((chunks, 2)),
            dma((chunks, 2)),
            dma((chunks, 2)),
            dma((xcount, groups)),
            dma((xcount, groups)),
        ],
        compiler_params=pltpu.CompilerParams(
            collective_id=0, has_side_effects=True, vmem_limit_bytes=60 * 1024 * 1024
        ),
        name="sweep_attention",
    )(
        queries,
        query_gain,
        cache_keys,
        cache_values,
        finished_keys,
        finished_values,
        new_keys,
        new_values,
        out_weight,
        time_weight,
        owner,
        step,
    )
    if aligned:
        return result
    summed = lax.psum_scatter(result, "head", scatter_dimension=1, tiled=True)
    half = freq // 2
    frequency = jnp.exp(-jnp.log(10000.0) * jnp.arange(half, dtype=F32) / half)
    phases = step[0].astype(F32) * frequency
    embedding = jnp.concatenate([jnp.cos(phases), jnp.sin(phases)])
    time_gate = 1.0 + jnp.dot(embedding, time_weight, precision=lax.Precision.HIGHEST)
    return (time_gate * summed).astype(BF16)


def solution(mesh):
    in_specs = (
        P(("grp", "seq"), "head"),
        P("head"),
        P(("grp", "slab"), "head"),
        P(("grp", "slab"), "head"),
        P(("grp", "slab", "seq"), "head"),
        P(("grp", "slab", "seq"), "head"),
        P(("grp", "slab", "seq"), "head"),
        P(("grp", "slab", "seq"), "head"),
        P("head", "slab"),
        P(None, ("slab", "head")),
        P("grp"),
        P("grp"),
    )
    out_specs = P(("grp", "seq"), ("slab", "head"))
    sizes = (mesh.shape["slab"], mesh.shape["head"], mesh.shape["seq"])
    return jax.shard_map(
        functools.partial(local, sizes),
        mesh=mesh,
        in_specs=in_specs,
        out_specs=out_specs,
        check_vma=False,
    )
```

```python
import functools
import math

import jax
import jax.numpy as jnp
from jax import lax
from jax.experimental import pallas as pl
from jax.experimental.pallas import tpu as pltpu
from jax.sharding import PartitionSpec as P

HEADS = 40
HD = 128
EPSILON = 1e-06
LOW = -1e30
LAG = 5
MESH = pl.DeviceIdType.MESH
F32 = jnp.float32
BF16 = jnp.bfloat16


def kernel(
    dims,
    aligned,
    q_ref,
    gain_ref,
    ck_ref,
    cv_ref,
    fk_ref,
    fv_ref,
    nk_ref,
    nv_ref,
    w_ref,
    tw_ref,
    owner_ref,
    step_ref,
    out_ref,
    q,
    qg,
    gain,
    kc,
    vc,
    kf,
    vf,
    w,
    tw,
    squares,
    scale,
    own_o,
    own_s,
    pre_o,
    pre_s,
    suf_o,
    suf_s,
    right_o,
    right_s,
    left_o,
    left_s,
    att,
    acc,
    gate,
    xs,
    xr,
    load_sem,
    fresh_sem,
    fresh_send,
    fresh_recv,
    sq_send,
    sq_recv,
    right_send,
    right_recv,
    left_send,
    left_recv,
    x_send,
    x_recv,
):
    n, heads_n, seq_n = dims
    rows, width = q_ref.shape
    hcount = width // HD
    z = lax.axis_index("slab")
    hx = lax.axis_index("head")
    sq = lax.axis_index("seq")

    groups = rows // HD
    chunks = groups * hcount
    loads = [
        pltpu.make_async_copy(src, dst, load_sem.at[i])
        for i, (src, dst) in enumerate(
            [(q_ref, q), (gain_ref, gain), (ck_ref, kc), (cv_ref, vc), (w_ref, w), (tw_ref, tw)]
        )
    ]
    loads[0].start()
    loads[1].start()
    barrier = pltpu.get_barrier_semaphore()
    for d in range(1, seq_n):
        pl.semaphore_signal(
            barrier, inc=1, device_id={"seq": lax.rem(sq + d, seq_n)}, device_id_type=MESH
        )
    for d in range(1, heads_n):
        pl.semaphore_signal(
            barrier, inc=1, device_id={"head": lax.rem(hx + d, heads_n)}, device_id_type=MESH
        )

    @pl.when(z > 0)
    def _():
        pl.semaphore_signal(barrier, inc=1, device_id={"slab": z - 1}, device_id_type=MESH)

    @pl.when(z < n - 1)
    def _():
        pl.semaphore_signal(barrier, inc=1, device_id={"slab": z + 1}, device_id_type=MESH)

    def clear(o_ref, s_ref):
        o_ref[...] = jnp.zeros_like(o_ref)
        s_ref[:, 0:1, :] = jnp.full((chunks, 1, HD), LOW, F32)
        s_ref[:, 1:2, :] = jnp.zeros((chunks, 1, HD), F32)

    @pl.when(z == 0)
    def _():
        clear(pre_o, pre_s)

    @pl.when(z == n - 1)
    def _():
        clear(suf_o, suf_s)

    ends = (z == 0).astype(jnp.int32) + (z == n - 1).astype(jnp.int32)
    pl.semaphore_wait(barrier, seq_n - 1 + heads_n - 1 + 2 - ends)

    fresh_src = [(fk_ref, kf, 0), (nk_ref, kf, 1), (fv_ref, vf, 0), (nv_ref, vf, 1)]
    first = max(hcount // 5, 1) * HD
    cuts = [slice(0, first), slice(first, width)]
    fresh_remote = [[], []]
    for k, cols in enumerate(cuts):
        for d in range(1, seq_n):
            for i, (src, dst, part) in enumerate(fresh_src):
                c = pltpu.make_async_remote_copy(
                    src_ref=src.at[:, cols],
                    dst_ref=dst.at[sq, part, :, cols],
                    send_sem=fresh_send.at[d - 1, k, i],
                    recv_sem=fresh_recv.at[d - 1, k, i],
                    device_id={"seq": lax.rem(sq + d, seq_n)},
                    device_id_type=MESH,
                )
                c.start()
                fresh_remote[k].append(c)

    loads[0].wait()
    loads[1].wait()
    loads[5].start()
    loads[2].start()
    loads[3].start()
    fresh_local = []
    for i, (src, dst, part) in enumerate(fresh_src):
        c = pltpu.make_async_copy(src, dst.at[sq, part], fresh_sem.at[i])
        c.start()
        fresh_local.append(c)
    loads[4].start()

    def squares_step(h, total):
        cols = pl.ds(pl.multiple_of(h * HD, HD), HD)
        x = q[:, cols].astype(F32)
        qg[:, cols] = (x * gain[cols][None, :]).astype(BF16)
        return total + x * x

    total = lax.fori_loop(0, hcount, squares_step, jnp.zeros((rows, HD), F32))
    row_total = jnp.sum(total.T, axis=0, keepdims=True)
    squares[hx] = jnp.broadcast_to(row_total, (8, rows))
    loads[5].wait()
    sq_copies = []
    for d in range(1, heads_n):
        c = pltpu.make_async_remote_copy(
            src_ref=squares.at[hx],
            dst_ref=squares.at[hx],
            send_sem=sq_send.at[d - 1],
            recv_sem=sq_recv.at[d - 1],
            device_id={"head": lax.rem(hx + d, heads_n)},
            device_id_type=MESH,
        )
        c.start()
        sq_copies.append(c)
    if aligned:
        half = tw.shape[0] // 2
        j = lax.broadcasted_iota(jnp.int32, (half, HD), 0).astype(F32)
        frequency = jnp.exp(F32(-math.log(10000.0)) * j / half)
        phases = jnp.full((half, HD), step_ref[0], jnp.int32).astype(F32) * frequency
        cos, sin = jnp.cos(phases), jnp.sin(phases)
        for c in range(tw.shape[1] // HD):
            cols = slice(c * HD, (c + 1) * HD)
            terms = tw[:half, cols] * cos + tw[half:, cols] * sin
            gate[:, cols] = 1.0 + jnp.sum(terms, axis=0, keepdims=True)

    for c in fresh_local + loads[2:4]:
        c.wait()
    for c in fresh_remote[0]:
        c.wait_recv()
    for c in sq_copies:
        c.wait_recv()
    norm_total = jnp.sum(squares[...], axis=0)
    scale[...] = lax.rsqrt(norm_total / (HEADS * HD) + EPSILON) * (
        math.log2(math.e) / HD**0.5
    )
    def send(h, direction):
        if direction > 0:
            pairs, ss, rs = ((right_o, pre_o), (right_s, pre_s)), right_send, right_recv
        else:
            pairs, ss, rs = ((left_o, suf_o), (left_s, suf_s)), left_send, left_recv
        return [
            pltpu.make_async_remote_copy(
                src_ref=src.at[h],
                dst_ref=dst.at[h],
                send_sem=ss.at[h, i],
                recv_sem=rs.at[h, i],
                device_id={"slab": z + direction},
                device_id_type=MESH,
            )
            for i, (src, dst) in enumerate(pairs)
        ]

    pair = 2 if hcount % 2 == 0 else 1
    fresh_rows = seq_n * 2 * fk_ref.shape[0]
    lag_end = LAG * jnp.maximum(z, n - 1 - z)

    def combine(h, other_o, other_s, dest_o, dest_s):
        m_a, l_a = own_s[h, 0:1], own_s[h, 1:2]
        m_b, l_b = other_s[h, 0:1], other_s[h, 1:2]
        top = jnp.maximum(m_a, m_b)
        e_a, e_b = jnp.exp2(m_a - top), jnp.exp2(m_b - top)
        dest_o[h] = (own_o[h] * e_a + other_o[h].astype(F32) * e_b).astype(BF16)
        dest_s[h, 0:1] = top
        dest_s[h, 1:2] = l_a * e_a + l_b * e_b

    nt = (((1,), (1,)), ((), ()))
    tn = (((0,), (0,)), ((), ()))

    def attend(h):
        cols = pl.ds(pl.multiple_of(h * HD, HD), HD)
        penalty = jnp.where(
            jnp.full((1, rows), owner_ref[0], jnp.int32) == z, F32(LOW), F32(0.0)
        )
        q_head = qg[:, cols]
        s_row = scale[0:1]
        s_c = (
            lax.dot_general(kc[:, cols], q_head, nt, preferred_element_type=F32) * s_row
            + penalty
        )
        k_fresh = kf[:, :, :, cols].reshape(fresh_rows, HD)
        v_fresh = vf[:, :, :, cols].reshape(fresh_rows, HD)
        s_f = lax.dot_general(k_fresh, q_head, nt, preferred_element_type=F32) * s_row
        top = jnp.maximum(
            jnp.max(s_c, axis=0, keepdims=True), jnp.max(s_f, axis=0, keepdims=True)
        )
        p_c = jnp.exp2(s_c - top)
        p_f = jnp.exp2(s_f - top)
        mass = jnp.sum(p_c, axis=0, keepdims=True) + jnp.sum(p_f, axis=0, keepdims=True)
        o = lax.dot_general(
            vc[:, cols], p_c.astype(BF16), tn, preferred_element_type=F32
        ) + lax.dot_general(v_fresh, p_f.astype(BF16), tn, preferred_element_type=F32)
        for g in range(groups):
            part = slice(g * HD, (g + 1) * HD)
            own_s[g * hcount + h, 0:1] = top[:, part]
            own_s[g * hcount + h, 1:2] = mass[:, part]
            own_o[g * hcount + h] = o[:, part]

    def project(g, p):
        deep = pl.ds(pl.multiple_of(p * pair * HD, HD), pair * HD)
        term = lax.dot_general(att[g, deep, :], w[deep, :], tn, preferred_element_type=F32)

        @pl.when(p == 0)
        def _():
            acc[g] = term

        @pl.when(p > 0)
        def _():
            acc[g] += term

    def exchange(g):
        copies = []
        for d in range(1, heads_n):
            copies.append(
                pltpu.make_async_remote_copy(
                    src_ref=xs.at[d - 1, g],
                    dst_ref=xr.at[d - 1, g],
                    send_sem=x_send.at[d - 1, g],
                    recv_sem=x_recv.at[d - 1, g],
                    device_id={"head": lax.rem(hx + d, heads_n)},
                    device_id_type=MESH,
                )
            )
        return copies

    def exchange_start(g):
        cp = out_ref.shape[1]
        for d, c in enumerate(exchange(g)):
            peer = lax.rem(hx + d + 1, heads_n)
            cols = pl.ds(pl.multiple_of(peer * cp, HD), cp)
            xs[d, g] = acc[g, :, cols].astype(BF16)
            c.start()

    pairs = hcount // pair
    last = (groups - 1) * hcount
    attend(0)

    def body(t, carry):
        cp_ = t - LAG * z
        in_p = (cp_ >= 0) & (cp_ < chunks)
        cs = t - LAG * (n - 1 - z)
        in_s = (cs >= 0) & (cs < chunks)

        @pl.when(in_p & (z > 0))
        def _():
            for c in send(cp_, 1):
                c.wait_recv()

        @pl.when(in_p & (z < n - 1))
        def _():
            combine(cp_, pre_o, pre_s, right_o, right_s)

        @pl.when(in_s & (z < n - 1))
        def _():
            for c in send(cs, -1):
                c.wait_recv()

        @pl.when(in_s & (z > 0))
        def _():
            combine(cs, suf_o, suf_s, left_o, left_s)

        f = t - lag_end

        @pl.when((f >= 0) & (f < chunks))
        def _():
            m_a, m_b, m_c = own_s[f, 0:1], pre_s[f, 0:1], suf_s[f, 0:1]
            top = jnp.maximum(m_a, jnp.maximum(m_b, m_c))
            e_a, e_b, e_c = jnp.exp2(m_a - top), jnp.exp2(m_b - top), jnp.exp2(m_c - top)
            mass = own_s[f, 1:2] * e_a + pre_s[f, 1:2] * e_b + suf_s[f, 1:2] * e_c
            total_o = (
                own_o[f] * e_a + pre_o[f].astype(F32) * e_b + suf_o[f].astype(F32) * e_c
            )
            h = lax.rem(f, hcount)
            att[f // hcount, pl.ds(pl.multiple_of(h * HD, HD), HD), :] = (
                total_o / mass
            ).astype(BF16)

        @pl.when(in_p & (z < n - 1))
        def _():
            for c in send(cp_, 1):
                c.start()

        @pl.when(in_s & (z > 0))
        def _():
            for c in send(cs, -1):
                c.start()

        @pl.when(t + 1 == first // HD)
        def _():
            for c in fresh_remote[1]:
                c.wait_recv()

        @pl.when(t + 1 < hcount)
        def _():
            attend(t + 1)

        @pl.when(f == last)
        def _():
            loads[4].wait()

        for g in range(groups - 1):

            @pl.when((f >= last) & (f < last + pairs))
            def _(g=g):
                project(g, f - last)

            if aligned:

                @pl.when(f == last + pairs - 1)
                def _(g=g):
                    exchange_start(g)

        done = f - last + 1

        @pl.when((done > 0) & (done <= hcount) & (lax.rem(done, pair) == 0))
        def _():
            project(groups - 1, done // pair - 1)

        return carry

    lax.fori_loop(0, chunks + LAG * (n - 1), body, 0)

    if aligned:
        cp = out_ref.shape[1]
        mine = pl.ds(pl.multiple_of(hx * cp, HD), cp)
        exchange_start(groups - 1)
        for g in range(groups):
            summed = acc[g, :, mine]
            for d, c in enumerate(exchange(g)):
                c.wait_recv()
                summed = summed + xr[d, g].astype(F32)
            out_ref[g * HD : (g + 1) * HD, :] = (summed * gate[...]).astype(out_ref.dtype)
        for g in range(groups):
            for c in exchange(g):
                c.wait_send()
    else:
        for g in range(groups):
            out_ref[g * HD : (g + 1) * HD, :] = acc[g]

    for c in fresh_remote[0] + fresh_remote[1] + sq_copies:
        c.wait_send()

    def drain(h, carry):
        @pl.when(z < n - 1)
        def _():
            for c in send(h, 1):
                c.wait_send()

        @pl.when(z > 0)
        def _():
            for c in send(h, -1):
                c.wait_send()

        return carry

    lax.fori_loop(0, chunks, drain, 0)


def local(sizes, *args):
    (
        queries,
        query_gain,
        cache_keys,
        cache_values,
        finished_keys,
        finished_values,
        new_keys,
        new_values,
        out_weight,
        time_weight,
        owner,
        step,
    ) = args
    n, heads_n, seq_n = sizes
    rows, width = queries.shape
    hcount = width // HD
    cached, fresh = cache_keys.shape[0], finished_keys.shape[0]
    columns, cp = out_weight.shape[1], time_weight.shape[1]
    freq = time_weight.shape[0]
    aligned = cp % HD == 0
    any_spec = pl.BlockSpec(memory_space=pl.ANY)
    smem = pl.BlockSpec(memory_space=pltpu.SMEM)
    vmem = pl.BlockSpec(memory_space=pltpu.VMEM)
    dma = pltpu.SemaphoreType.DMA
    xcount = max(heads_n - 1, 1)
    groups = rows // HD
    chunks = groups * hcount
    stat = (chunks, 2, HD)
    part = (chunks, HD, HD)
    result = pl.pallas_call(
        functools.partial(kernel, sizes, aligned),
        out_shape=jax.ShapeDtypeStruct(
            (rows, cp if aligned else columns), BF16 if aligned else F32
        ),
        in_specs=[any_spec] * 10 + [smem] * 2,
        out_specs=vmem,
        scratch_shapes=[
            pltpu.VMEM((rows, width), BF16),
            pltpu.VMEM((rows, width), BF16),
            pltpu.VMEM((width,), F32),
            pltpu.VMEM((cached, width), BF16),
            pltpu.VMEM((cached, width), BF16),
            pltpu.VMEM((seq_n, 2, fresh, width), BF16),
            pltpu.VMEM((seq_n, 2, fresh, width), BF16),
            pltpu.VMEM((width, columns), BF16),
            pltpu.VMEM((freq, cp), F32),
            pltpu.VMEM((heads_n, 8, rows), F32),
            pltpu.VMEM((8, rows), F32),
            pltpu.VMEM(part, F32),
            pltpu.VMEM(stat, F32),
            pltpu.VMEM(part, BF16),
            pltpu.VMEM(stat, F32),
            pltpu.VMEM(part, BF16),
            pltpu.VMEM(stat, F32),
            pltpu.VMEM(part, BF16),
            pltpu.VMEM(stat, F32),
            pltpu.VMEM(part, BF16),
            pltpu.VMEM(stat, F32),
            pltpu.VMEM((groups, width, HD), BF16),
            pltpu.VMEM((groups, HD, columns), F32),
            pltpu.VMEM((1, cp), F32),
            pltpu.VMEM((xcount, groups, HD, cp), BF16),
            pltpu.VMEM((xcount, groups, HD, cp), BF16),
            dma((6,)),
            dma((4,)),
            dma((max(seq_n - 1, 1), 2, 4)),
            dma((max(seq_n - 1, 1), 2, 4)),
            dma((xcount,)),
            dma((xcount,)),
            dma((chunks, 2)),
            dma((chunks, 2)),
            dma((chunks, 2)),
            dma((chunks, 2)),
            dma((xcount, groups)),
            dma((xcount, groups)),
        ],
        compiler_params=pltpu.CompilerParams(
            collective_id=0, has_side_effects=True, vmem_limit_bytes=60 * 1024 * 1024
        ),
        name="sweep_attention",
    )(
        queries,
        query_gain,
        cache_keys,
        cache_values,
        finished_keys,
        finished_values,
        new_keys,
        new_values,
        out_weight,
        time_weight,
        owner,
        step,
    )
    if aligned:
        return result
    summed = lax.psum_scatter(result, "head", scatter_dimension=1, tiled=True)
    half = freq // 2
    frequency = jnp.exp(-jnp.log(10000.0) * jnp.arange(half, dtype=F32) / half)
    phases = step[0].astype(F32) * frequency
    embedding = jnp.concatenate([jnp.cos(phases), jnp.sin(phases)])
    time_gate = 1.0 + jnp.dot(embedding, time_weight, precision=lax.Precision.HIGHEST)
    return (time_gate * summed).astype(BF16)


def solution(mesh):
    in_specs = (
        P(("grp", "seq"), "head"),
        P("head"),
        P(("grp", "slab"), "head"),
        P(("grp", "slab"), "head"),
        P(("grp", "slab", "seq"), "head"),
        P(("grp", "slab", "seq"), "head"),
        P(("grp", "slab", "seq"), "head"),
        P(("grp", "slab", "seq"), "head"),
        P("head", "slab"),
        P(None, ("slab", "head")),
        P("grp"),
        P("grp"),
    )
    out_specs = P(("grp", "seq"), ("slab", "head"))
    sizes = (mesh.shape["slab"], mesh.shape["head"], mesh.shape["seq"])
    return jax.shard_map(
        functools.partial(local, sizes),
        mesh=mesh,
        in_specs=in_specs,
        out_specs=out_specs,
        check_vma=False,
    )
```
